128 devices in a mesh: gy: 4 (over z_lo, core), gx: 32 (over z_hi, y, x).
Axes of the slice: x: 4, y: 4, z: 4 (z_hi: 2, z_lo: 2; z = z_hi * 2 + z_lo), core: 2. Of those that a mesh axis runs over, the one named last changes fastest.
Arguments:
- first_factor: bfloat16 [4096, 8192], P('gy', 'gx'), may hold values from -6 to 6
- second_factor: bfloat16 [8192, 32768], P('gy', 'gx'), may hold values from -0.0625 to 0.0625
- result_in: float32 [4096, 32768], P('gy', 'gx'), may hold values from -6 to 6
- pivot_scale: float32 [8192], replicated, may hold values from 0.25 to 1.75
Outputs:
- corrected: float32 [4096, 32768], P('gy', 'gx')
The draws below stay inside these ranges and needn't reach their ends.
All inputs are finite; a program needn't handle non-finite values.
Results may differ from the reference program's by a relative error of at most 0.002.
Values may be sent and summed in bfloat16 or wider, within the bound.
No kernel may reach another device: no remote copies, remote signals or barrier semaphores. Data moves between devices by JAX's collectives and lax.ppermute only.
A program may use at most 128 MiB of HBM per device.

```python
import jax
import jax.numpy as jnp
from jax import lax

ROWS = 4096
COLS = 32768
INNER = 8192


def levels(rng, dims, shards, low, largest):
    def one(dim, blocks):
        draws = jax.random.uniform(jax.random.fold_in(jax.random.fold_in(rng, 6), dim), (blocks,), jnp.float32, low / len(shards), largest / len(shards))
        return jnp.repeat(jnp.exp(draws), dims[dim] // blocks).reshape((-1,) + (1,) * (len(dims) - dim - 1))

    factor_of = one(*shards[0])
    for cut in shards[1:]:
        factor_of = factor_of * one(*cut)
    return factor_of


def centred(rng, extent, spread, most, pieces=(), held_as=jnp.bfloat16):
    loudness = levels(rng, extent, pieces, -0.22, 0.18) if pieces else 1.0
    drawn = jax.random.normal(rng, extent, jnp.float32) * spread * loudness
    return jnp.minimum(jnp.maximum(drawn, -most), most).astype(held_as)


def setup_inputs(seed: int = 0) -> dict:
    keys = jax.random.split(jax.random.key(seed), 5)
    first_factor = centred(keys[0], (ROWS, INNER), 1.0, 6.0, ((0, 4), (1, 32)))
    second_factor = centred(keys[1], (INNER, COLS), INNER ** -0.5, 0.0625, ((0, 4), (1, 32)))
    result_in = centred(keys[2], (ROWS, COLS), 1.0, 6.0, ((0, 4), (1, 32)), jnp.float32)
    pivot_scale = jnp.clip(1.0 + 0.15 * jax.random.normal(keys[3], (INNER,), jnp.float32), 0.25, 1.75)
    return dict(first_factor=first_factor, second_factor=second_factor, result_in=result_in, pivot_scale=pivot_scale)


def reference(first_factor, second_factor, result_in, pivot_scale):
    scaled_left = (first_factor.astype(jnp.float32) * pivot_scale).astype(jnp.bfloat16)
    corrected = result_in - jnp.dot(scaled_left, second_factor, preferred_element_type=jnp.float32)
    row_power = lax.optimization_barrier(jnp.sum(corrected * corrected, axis=1))
    corrected = corrected * lax.rsqrt(row_power / COLS + 1e-06)[:, None]
    return corrected
```

```python
import functools

import jax
import jax.numpy as jnp
from jax import lax
from jax.experimental import pallas as pl
from jax.experimental.pallas import tpu as pltpu
from jax.sharding import Mesh, PartitionSpec as P


RING = 4
WIDTH = 256


def flip_low(i):
    return i ^ 1


def flip_high(i):
    return RING - 1 - i


def exchange(block, axis, step):
    pairs = []
    for core in range(2):
        partner = flip_low if (core + step) % 2 == 0 else flip_high
        pairs += [(core * RING + i, core * RING + partner(i)) for i in range(RING)]
    return lax.ppermute(block, ("c", axis), pairs)


def spread(own, first, second):
    held = own
    for axis, step in ((first, 0), (first, 1), (second, 0)):
        held = jnp.concatenate([held, exchange(held, axis, step)])
    return held, exchange(held, second, 1)


def ring_slots(me, core):
    low, high = flip_low(me), flip_high(me)
    one = jnp.where(core == 0, low, high)
    two = jnp.where(core == 0, high, low)
    across = (me + 2) % RING
    return [me, one, two, across]


def slot_columns(slot, x_first):
    core = lax.axis_index("c")
    xs = ring_slots(lax.axis_index("x"), core)
    ys = ring_slots(lax.axis_index("y"), core)
    if x_first:
        x, y = xs[slot % RING], ys[slot // RING]
    else:
        x, y = xs[slot // RING], ys[slot % RING]
    mine = (y // 2) == core
    index = (y % 2) * RING + x + jnp.where(mine, 0, 8)
    return pl.multiple_of(index * WIDTH, WIDTH)


def load_left(parts, left, sems):
    rows = left.shape[0] // 2
    copies = []
    for colour in range(2):
        for slot in range(16):
            source = parts[colour * 2 + slot // 8].at[slot % 8]
            columns = slot_columns(slot, colour == 0)
            copies.append(
                pltpu.make_async_copy(
                    source,
                    left.at[pl.ds(colour * rows, rows), pl.ds(columns, WIDTH)],
                    sems.at[colour * 16 + slot],
                )
            )
    return copies


def partial_kernel(x0, x1, y0, y1, mine_ref, other_ref, out_ref, left, sems):
    @pl.when(pl.program_id(0) == 0)
    def _():
        copies = load_left((x0, x1, y0, y1), left, sems)
        for copy in copies:
            copy.start()
        for copy in copies:
            copy.wait()

    depth = mine_ref.shape[0]
    total = jnp.dot(left[:, :depth], mine_ref[...], preferred_element_type=jnp.float32)
    total += jnp.dot(left[:, depth:], other_ref[...], preferred_element_type=jnp.float32)
    out_ref[...] = total.astype(out_ref.dtype)


def final_kernel(
    x0, x1, y0, y1, mine_ref, other_ref, result_ref, sent_ref, out_ref, power_ref, left, power, sems
):
    step = pl.program_id(0)

    @pl.when(step == 0)
    def _():
        copies = load_left((x0, x1, y0, y1), left, sems)
        for copy in copies:
            copy.start()
        power[...] = jnp.zeros_like(power)
        for copy in copies:
            copy.wait()

    depth = mine_ref.shape[0]
    total = jnp.dot(left[:, :depth], mine_ref[...], preferred_element_type=jnp.float32)
    total += jnp.dot(left[:, depth:], other_ref[...], preferred_element_type=jnp.float32)
    corrected = result_ref[...] - (total + sent_ref[...].astype(jnp.float32))
    out_ref[...] = corrected
    squares = corrected * corrected
    lanes = power.shape[1]
    for i in range(squares.shape[1] // lanes):
        power[...] += squares[:, i * lanes : (i + 1) * lanes]

    @pl.when(step == pl.num_programs(0) - 1)
    def _():
        for i in range(power.shape[0] // lanes):
            block = power[i * lanes : (i + 1) * lanes, :]
            power_ref[i : i + 1, :] = jnp.sum(block.T, axis=0, keepdims=True)


def scale_kernel(columns, power_ref, corrected_ref, out_ref, factor):
    lanes = power_ref.shape[-1]
    row_power = jnp.sum(power_ref[...], axis=0)
    inverse = lax.rsqrt(row_power / columns + 1e-06)
    step = pl.program_id(0)
    del step
    for i in range(inverse.shape[0]):
        factor[...] = jnp.broadcast_to(inverse[i : i + 1, :], (lanes, lanes)).T
        for j in range(out_ref.shape[1] // lanes):
            here = (slice(i * lanes, (i + 1) * lanes), slice(j * lanes, (j + 1) * lanes))
            out_ref[here] = corrected_ref[here] * factor[...]


def matmul_cost(rows, depth, columns, extra):
    return pl.CostEstimate(
        flops=2 * rows * depth * columns,
        bytes_accessed=2 * (rows * depth + depth * columns) + extra,
        transcendentals=0,
    )


ANY = pl.BlockSpec(memory_space=pl.ANY)


def shards(first_factor, second_factor, result_in, pivot_scale):
    rows, width = first_factor.shape
    depth, columns = second_factor.shape
    half = rows // 2
    tile = 256
    hi, lo = lax.axis_index("hi"), lax.axis_index("lo")
    place = (hi * 4 + lax.axis_index("y")) * 4 + lax.axis_index("x")
    part_scale = lax.dynamic_slice_in_dim(pivot_scale, place * width, width)
    scaled = (first_factor.astype(jnp.float32) * part_scale).astype(jnp.bfloat16)

    near = hi == lo
    to_ends = lax.ppermute(scaled, ("lo", "hi"), [(2, 0), (1, 3)])
    to_middle = lax.ppermute(scaled, ("lo", "hi"), [(2, 1), (1, 2)])
    foreign = jnp.where(near, to_ends, to_middle)
    across = lax.ppermute(scaled, ("lo", "hi"), [(0, 1), (3, 2)])
    native = jnp.where(near, scaled, across)
    other = lax.ppermute(second_factor, "c", [(0, 1), (1, 0)])

    def gathered(block):
        x0, x1 = spread(block[None, :half], "x", "y")
        y0, y1 = spread(block[None, half:], "y", "x")
        return x0, x1, y0, y1

    right_spec = pl.BlockSpec((depth, tile), lambda j: (0, j))
    tile_spec = pl.BlockSpec((rows, tile), lambda j: (0, j))
    scratch = [pltpu.VMEM((rows, 2 * depth), jnp.bfloat16)]
    sems = [pltpu.SemaphoreType.DMA((32,))]
    params = pltpu.CompilerParams(vmem_limit_bytes=40 * 2**20)

    partial = pl.pallas_call(
        partial_kernel,
        grid=(columns // tile,),
        out_shape=jax.ShapeDtypeStruct((rows, columns), jnp.bfloat16),
        in_specs=[ANY] * 4 + [right_spec] * 2,
        out_specs=tile_spec,
        scratch_shapes=scratch + sems,
        compiler_params=params,
        cost_estimate=matmul_cost(rows, 2 * depth, columns, rows * columns * 2),
        name="partial",
    )(*gathered(foreign), second_factor, other)
    sent = lax.ppermute(partial, "lo", [(0, 1), (1, 0)])

    corrected, power = pl.pallas_call(
        final_kernel,
        grid=(columns // tile,),
        out_shape=(
            jax.ShapeDtypeStruct((rows, columns), jnp.float32),
            jax.ShapeDtypeStruct((rows // 128, 128), jnp.float32),
        ),
        in_specs=[ANY] * 4 + [right_spec] * 2 + [tile_spec] * 2,
        out_specs=(tile_spec, pl.BlockSpec((rows // 128, 128), lambda j: (0, 0))),
        scratch_shapes=scratch + [pltpu.VMEM((rows, 128), jnp.float32)] + sems,
        compiler_params=params,
        cost_estimate=matmul_cost(rows, 2 * depth, columns, rows * columns * 10),
        name="final",
    )(*gathered(native), second_factor, other, result_in, sent)

    line = lax.axis_size(("hi", "y", "x"))
    copies = jnp.broadcast_to(power, (line, *power.shape))
    powers = lax.all_to_all(copies, ("hi", "y", "x"), split_axis=0, concat_axis=0, tiled=True)

    scale_spec = pl.BlockSpec((rows, tile), lambda j: (0, j))
    return pl.pallas_call(
        functools.partial(scale_kernel, columns * line),
        grid=(columns // tile,),
        out_shape=jax.ShapeDtypeStruct((rows, columns), jnp.float32),
        in_specs=[pl.BlockSpec(powers.shape, lambda j: (0, 0, 0)), scale_spec],
        out_specs=scale_spec,
        scratch_shapes=[pltpu.VMEM((128, 128), jnp.float32)],
        compiler_params=params,
        name="scale",
    )(powers, corrected)


def solution(mesh):
    parts = Mesh(mesh.devices.reshape(2, 2, 2, 4, 4), ("lo", "c", "hi", "y", "x"))
    spec = P(("lo", "c"), ("hi", "y", "x"))
    return jax.shard_map(
        shards, mesh=parts, in_specs=(spec, spec, spec, P()), out_specs=spec, check_vma=False
    )
```

```python
import functools

import jax
import jax.numpy as jnp
from jax import lax
from jax.experimental import pallas as pl
from jax.experimental.pallas import tpu as pltpu
from jax.sharding import Mesh, PartitionSpec as P


RING = 4
WIDTH = 256


def flip_low(i):
    return i ^ 1


def flip_high(i):
    return RING - 1 - i


def exchange(block, axis, step):
    pairs = []
    for core in range(2):
        partner = flip_low if (core + step) % 2 == 0 else flip_high
        pairs += [(core * RING + i, core * RING + partner(i)) for i in range(RING)]
    return lax.ppermute(block, ("c", axis), pairs)


def joined(held, arrived):
    return jnp.concatenate([held, arrived])


def spread_line(own, axis):
    held = own
    for k in range(2):
        held = joined(held, exchange(held, axis, k))
    return held


def spread_plane(held, second):
    held = joined(held, exchange(held, second, 0))
    return held, exchange(held, second, 1)


def ring_slots(me, core):
    low, high = flip_low(me), flip_high(me)
    one = jnp.where(core == 0, low, high)
    two = jnp.where(core == 0, high, low)
    across = (me + 2) % RING
    return [me, one, two, across]


def slot_columns(slot, x_first):
    core = lax.axis_index("c")
    xs = ring_slots(lax.axis_index("x"), core)
    ys = ring_slots(lax.axis_index("y"), core)
    if x_first:
        x, y = xs[slot % RING], ys[slot // RING]
    else:
        x, y = xs[slot // RING], ys[slot % RING]
    mine = (y // 2) == core
    return ((y % 2) * RING + x + jnp.where(mine, 0, 8)) * WIDTH


def load_left(parts, left, sems):
    rows = left.shape[0] // 2
    copies = []
    for colour in range(2):
        for slot in range(16):
            source = parts[colour * 2 + slot // 8].at[slot % 8]
            columns = pl.multiple_of(slot_columns(slot, colour == 0), WIDTH)
            copies.append(
                pltpu.make_async_copy(
                    source,
                    left.at[pl.ds(colour * rows, rows), pl.ds(columns, WIDTH)],
                    sems.at[colour * 16 + slot],
                )
            )
    return copies


def load_slots(parts, left, sems):
    rows = left.shape[0] // 2
    return [
        pltpu.make_async_copy(
            parts[colour].at[slot],
            left.at[pl.ds(colour * rows, rows), pl.ds(slot * WIDTH, WIDTH)],
            sems.at[colour * 8 + slot],
        )
        for colour in range(2)
        for slot in range(8)
    ]


def product(left, right):
    return jnp.dot(left, right, preferred_element_type=jnp.float32)


def slot_product(left, mine, partner, colour, first_slot):
    rows = left.shape[0] // 2
    depth = mine.shape[0]
    total = None
    for slot in range(8):
        begin = slot_columns(first_slot + slot, colour == 0)
        here = pl.multiple_of(jnp.minimum(begin, depth - WIDTH), WIDTH)
        there = pl.multiple_of(jnp.maximum(begin - depth, 0), WIDTH)
        right = jnp.where(
            begin < depth, mine[pl.ds(here, WIDTH), :], partner[pl.ds(there, WIDTH), :]
        )
        term = product(
            left[colour * rows : (colour + 1) * rows, slot * WIDTH : (slot + 1) * WIDTH], right
        )
        total = term if total is None else total + term
    return total


def local_kernel(x0, y0, mine, partner, result_ref, out_ref, left, sems):
    @pl.when(pl.program_id(0) == 0)
    def _():
        copies = load_slots((x0, y0), left, sems)
        for copy in copies:
            copy.start()
        for copy in copies:
            copy.wait()

    rows = left.shape[0] // 2
    for colour in range(2):
        here = slice(colour * rows, (colour + 1) * rows)
        out_ref[here, :] = result_ref[here, :] - slot_product(left, mine, partner, colour, 0)


def remote_kernel(x0, x1, y0, y1, same, relayed, so_far, out_ref, rest_ref, left, sems):
    first = same.shape[0]
    depth = left.shape[1] // 2

    @pl.when(pl.program_id(0) == 0)
    def _():
        copies = load_left((x0, x1, y0, y1), left, sems)
        for copy in copies:
            copy.start()
        for copy in copies:
            copy.wait()
        rest_ref[:, : depth - first] = left[:, first:depth]
        rest_ref[:, depth - first :] = left[:, depth + first :]

    out_ref[...] = so_far[...] - (
        product(left[:, :first], same[...])
        + product(left[:, depth : depth + first], relayed[...])
    )


def final_kernel(
    x1, y1, mine, partner, rest, same, relayed, so_far, out_ref, power_ref, left, power, sems
):
    step = pl.program_id(0)
    last = same.shape[0]

    @pl.when(step == 0)
    def _():
        copies = load_slots((x1, y1), left, sems)
        for copy in copies:
            copy.start()
        power[...] = jnp.zeros_like(power)
        for copy in copies:
            copy.wait()

    rows = left.shape[0] // 2
    lanes = power.shape[1]
    for colour in range(2):
        here = slice(colour * rows, (colour + 1) * rows)
        total = slot_product(left, mine, partner, colour, 8)
        total += product(rest[here, :last], same[...]) + product(rest[here, last:], relayed[...])
        corrected = so_far[here, :] - total
        out_ref[here, :] = corrected
        squares = corrected * corrected
        for i in range(squares.shape[1] // lanes):
            power[here, :] += squares[:, i * lanes : (i + 1) * lanes]

    @pl.when(step == pl.num_programs(0) - 1)
    def _():
        for i in range(power.shape[0] // lanes):
            block = power[i * lanes : (i + 1) * lanes, :]
            power_ref[i : i + 1, :] = jnp.sum(block.T, axis=0, keepdims=True)


def scale_kernel(columns, power_ref, corrected_ref, out_ref, factor):
    lanes = power_ref.shape[-1]
    row_power = jnp.sum(power_ref[...], axis=0)
    inverse = lax.rsqrt(row_power / columns + 1e-06)
    step = pl.program_id(0)
    del step
    for i in range(inverse.shape[0]):
        factor[...] = jnp.broadcast_to(inverse[i : i + 1, :], (lanes, lanes)).T
        for j in range(out_ref.shape[1] // lanes):
            here = (slice(i * lanes, (i + 1) * lanes), slice(j * lanes, (j + 1) * lanes))
            out_ref[here] = corrected_ref[here] * factor[...]


def matmul_cost(rows, depth, columns, extra):
    return pl.CostEstimate(
        flops=2 * rows * depth * columns,
        bytes_accessed=2 * (rows * depth + depth * columns) + extra,
        transcendentals=0,
    )


ANY = pl.BlockSpec(memory_space=pl.ANY)


def shards(first_factor, second_factor, result_in, pivot_scale):
    rows, width = first_factor.shape
    depth, columns = second_factor.shape
    half = rows // 2
    tile = 256
    hi = lax.axis_index("hi")
    place = (hi * 4 + lax.axis_index("y")) * 4 + lax.axis_index("x")
    part_scale = lax.dynamic_slice_in_dim(pivot_scale, place * width, width)
    scaled = (first_factor.astype(jnp.float32) * part_scale).astype(jnp.bfloat16)

    foreign = lax.ppermute(scaled, "hi", [(0, 1), (1, 0)])

    first = depth * 3 // 4
    swap = [(0, 1), (1, 0)]
    same0 = lax.ppermute(second_factor[:first], "lo", swap)
    same1 = lax.ppermute(second_factor[first:], "lo", swap)
    partner = lax.ppermute(second_factor, "c", swap)
    relayed0 = lax.ppermute(same0, "c", swap)
    relayed1 = lax.ppermute(same1, "c", swap)

    def lines(block):
        return (spread_line(block[None, :half], "x"), spread_line(block[None, half:], "y"))

    def planes(line_x, line_y):
        return (*spread_plane(line_x, "y"), *spread_plane(line_y, "x"))

    near = hi == lax.axis_index("lo")
    native = lines(scaled)
    foreign = lines(foreign)
    remote_x0, remote_x1, remote_y0, remote_y1 = planes(
        *(jnp.where(near, f, n) for n, f in zip(native, foreign))
    )
    local_x0, local_x1, local_y0, local_y1 = planes(
        *(jnp.where(near, n, f) for n, f in zip(native, foreign))
    )

    def params(mebibytes):
        return pltpu.CompilerParams(vmem_limit_bytes=mebibytes * 2**20)

    def columns_of(array):
        return pl.BlockSpec((array.shape[0], tile), lambda j: (0, j))

    def whole(*shape):
        return pl.BlockSpec(shape, lambda j: (0,) * len(shape))

    grid = (columns // tile,)
    sums = jax.ShapeDtypeStruct((rows, columns), jnp.float32)
    tile_spec = columns_of(sums)
    eight_slots = [pltpu.VMEM((rows, 8 * WIDTH), jnp.bfloat16)]
    so_far = pl.pallas_call(
        local_kernel,
        grid=grid,
        out_shape=sums,
        in_specs=[ANY] * 2 + [columns_of(second_factor)] * 2 + [tile_spec],
        out_specs=tile_spec,
        scratch_shapes=eight_slots + [pltpu.SemaphoreType.DMA((16,))],
        compiler_params=params(16),
        cost_estimate=matmul_cost(rows, 8 * WIDTH, columns, rows * columns * 4),
        name="local",
    )(local_x0, local_y0, second_factor, partner, result_in)

    rest = 2 * (depth - first)
    so_far, left_over = pl.pallas_call(
        remote_kernel,
        grid=grid,
        out_shape=(sums, jax.ShapeDtypeStruct((rows, rest), jnp.bfloat16)),
        in_specs=[ANY] * 4 + [columns_of(same0), columns_of(relayed0), tile_spec],
        out_specs=(tile_spec, whole(rows, rest)),
        scratch_shapes=[
            pltpu.VMEM((rows, 2 * depth), jnp.bfloat16),
            pltpu.SemaphoreType.DMA((32,)),
        ],
        compiler_params=params(24),
        cost_estimate=matmul_cost(rows, 2 * first, columns, rows * columns * 8),
        name="remote",
    )(remote_x0, remote_x1, remote_y0, remote_y1, same0, relayed0, so_far)

    corrected, power = pl.pallas_call(
        final_kernel,
        grid=grid,
        out_shape=(sums, jax.ShapeDtypeStruct((rows // 128, 128), jnp.float32)),
        in_specs=[ANY] * 2
        + [columns_of(second_factor)] * 2
        + [whole(rows, rest), columns_of(same1), columns_of(relayed1), tile_spec],
        out_specs=(tile_spec, whole(rows // 128, 128)),
        scratch_shapes=eight_slots
        + [pltpu.VMEM((rows, 128), jnp.float32), pltpu.SemaphoreType.DMA((16,))],
        compiler_params=params(60),
        cost_estimate=matmul_cost(rows, 8 * WIDTH + rest, columns, rows * columns * 12),
        name="final",
    )(local_x1, local_y1, second_factor, partner, left_over, same1, relayed1, so_far)

    line = lax.axis_size(("hi", "y", "x"))
    copies = jnp.broadcast_to(power, (line, *power.shape))
    powers = lax.all_to_all(copies, ("hi", "y", "x"), split_axis=0, concat_axis=0, tiled=True)

    scale_spec = pl.BlockSpec((rows, tile), lambda j: (0, j))
    return pl.pallas_call(
        functools.partial(scale_kernel, columns * line),
        grid=(columns // tile,),
        out_shape=jax.ShapeDtypeStruct((rows, columns), jnp.float32),
        in_specs=[pl.BlockSpec(powers.shape, lambda j: (0, 0, 0)), scale_spec],
        out_specs=scale_spec,
        scratch_shapes=[pltpu.VMEM((128, 128), jnp.float32)],
        input_output_aliases={1: 0},
        compiler_params=params(12),
        name="scale",
    )(powers, corrected)


def solution(mesh):
    parts = Mesh(mesh.devices.reshape(2, 2, 2, 4, 4), ("lo", "c", "hi", "y", "x"))
    spec = P(("lo", "c"), ("hi", "y", "x"))

    return jax.shard_map(
        shards, mesh=parts, in_specs=(spec, spec, spec, P()), out_specs=spec, check_vma=False
    )
```

```python
import functools

import jax
import jax.numpy as jnp
from jax import lax
from jax.experimental import pallas as pl
from jax.experimental.pallas import tpu as pltpu
from jax.sharding import Mesh, PartitionSpec as P


RING = 4
WIDTH = 256


def flip_low(i):
    return i ^ 1


def flip_high(i):
    return RING - 1 - i


def exchange(block, axis, step):
    pairs = []
    for core in range(2):
        partner = flip_low if (core + step) % 2 == 0 else flip_high
        pairs += [(core * RING + i, core * RING + partner(i)) for i in range(RING)]
    return lax.ppermute(block, ("c", axis), pairs)


def joined(held, arrived):
    return jnp.concatenate([held, arrived])


def spread_line(own, axis):
    held = own
    for k in range(2):
        held = joined(held, exchange(held, axis, k))
    return held


def spread_plane(held, second):
    held = joined(held, exchange(held, second, 0))
    return held, exchange(held, second, 1)


def ring_slots(me, core):
    low, high = flip_low(me), flip_high(me)
    one = jnp.where(core == 0, low, high)
    two = jnp.where(core == 0, high, low)
    across = (me + 2) % RING
    return [me, one, two, across]


def slot_columns(slot, x_first):
    core = lax.axis_index("c")
    xs = ring_slots(lax.axis_index("x"), core)
    ys = ring_slots(lax.axis_index("y"), core)
    if x_first:
        x, y = xs[slot % RING], ys[slot // RING]
    else:
        x, y = xs[slot // RING], ys[slot % RING]
    mine = (y // 2) == core
    return ((y % 2) * RING + x + jnp.where(mine, 0, 8)) * WIDTH


def load_left(parts, left, sems):
    rows = left.shape[0] // 2
    copies = []
    for colour in range(2):
        for slot in range(16):
            source = parts[colour * 2 + slot // 8].at[slot % 8]
            columns = pl.multiple_of(slot_columns(slot, colour == 0), WIDTH)
            copies.append(
                pltpu.make_async_copy(
                    source,
                    left.at[pl.ds(colour * rows, rows), pl.ds(columns, WIDTH)],
                    sems.at[colour * 16 + slot],
                )
            )
    return copies


def product(left, right):
    return jnp.dot(left, right, preferred_element_type=jnp.float32)


def slot_product(left, local, colour, first_slot):
    total = None
    for slot in range(8):
        begin = pl.multiple_of(slot_columns(first_slot + slot, colour == 0), WIDTH)
        term = product(left[slot], local[pl.ds(begin, WIDTH), :])
        total = term if total is None else total + term
    return total


def local_kernel(x0, y0, local, result_ref, out_ref):
    rows = x0.shape[1]
    for colour, left in enumerate((x0, y0)):
        here = slice(colour * rows, (colour + 1) * rows)
        out_ref[here, :] = result_ref[here, :] - slot_product(left, local, colour, 0)


def remote_kernel(x0, x1, y0, y1, same, relayed, so_far, out_ref, rest_ref, left, sems):
    first = same.shape[0]
    depth = left.shape[1] // 2

    @pl.when(pl.program_id(0) == 0)
    def _():
        copies = load_left((x0, x1, y0, y1), left, sems)
        for copy in copies:
            copy.start()
        for copy in copies:
            copy.wait()
        rest_ref[:, : depth - first] = left[:, first:depth]
        rest_ref[:, depth - first :] = left[:, depth + first :]

    out_ref[...] = so_far[...] - (
        product(left[:, :first], same[...])
        + product(left[:, depth : depth + first], relayed[...])
    )


def final_kernel(x1, y1, local, rest, same, relayed, so_far, out_ref, power_ref, power):
    step = pl.program_id(0)
    last = same.shape[0]

    @pl.when(step == 0)
    def _():
        power[...] = jnp.zeros_like(power)

    rows = x1.shape[1]
    lanes = power.shape[1]
    for colour, left in enumerate((x1, y1)):
        here = slice(colour * rows, (colour + 1) * rows)
        total = slot_product(left, local, colour, 8)
        total += product(rest[here, :last], same[...]) + product(rest[here, last:], relayed[...])
        corrected = so_far[here, :] - total
        out_ref[here, :] = corrected
        squares = corrected * corrected
        for i in range(squares.shape[1] // lanes):
            power[here, :] += squares[:, i * lanes : (i + 1) * lanes]

    @pl.when(step == pl.num_programs(0) - 1)
    def _():
        for i in range(power.shape[0] // lanes):
            block = power[i * lanes : (i + 1) * lanes, :]
            power_ref[i : i + 1, :] = jnp.sum(block.T, axis=0, keepdims=True)


def scale_kernel(columns, power_ref, corrected_ref, out_ref, factor):
    lanes = power_ref.shape[-1]
    row_power = jnp.sum(power_ref[...], axis=0)
    inverse = lax.rsqrt(row_power / columns + 1e-06)
    step = pl.program_id(0)
    del step
    for i in range(inverse.shape[0]):
        factor[...] = jnp.broadcast_to(inverse[i : i + 1, :], (lanes, lanes)).T
        for j in range(out_ref.shape[1] // lanes):
            here = (slice(i * lanes, (i + 1) * lanes), slice(j * lanes, (j + 1) * lanes))
            out_ref[here] = corrected_ref[here] * factor[...]


def matmul_cost(rows, depth, columns, extra):
    return pl.CostEstimate(
        flops=2 * rows * depth * columns,
        bytes_accessed=2 * (rows * depth + depth * columns) + extra,
        transcendentals=0,
    )


ANY = pl.BlockSpec(memory_space=pl.ANY)


def shards(first_factor, second_factor, result_in, pivot_scale):
    rows, width = first_factor.shape
    depth, columns = second_factor.shape
    half = rows // 2
    tile = 256
    hi = lax.axis_index("hi")
    place = (hi * 4 + lax.axis_index("y")) * 4 + lax.axis_index("x")
    part_scale = lax.dynamic_slice_in_dim(pivot_scale, place * width, width)
    scaled = (first_factor.astype(jnp.float32) * part_scale).astype(jnp.bfloat16)

    foreign = lax.ppermute(scaled, "hi", [(0, 1), (1, 0)])

    first = depth * 3 // 4
    swap = [(0, 1), (1, 0)]
    same0 = lax.ppermute(second_factor[:first], "lo", swap)
    same1 = lax.ppermute(second_factor[first:], "lo", swap)
    partner = lax.ppermute(second_factor, "c", swap)
    relayed0 = lax.ppermute(same0, "c", swap)
    relayed1 = lax.ppermute(same1, "c", swap)

    local = jnp.concatenate([second_factor, partner])

    def lines(block):
        return (spread_line(block[None, :half], "x"), spread_line(block[None, half:], "y"))

    def planes(line_x, line_y):
        return (*spread_plane(line_x, "y"), *spread_plane(line_y, "x"))

    near = hi == lax.axis_index("lo")
    native = lines(scaled)
    foreign = lines(foreign)
    remote_x0, remote_x1, remote_y0, remote_y1 = planes(
        *(jnp.where(near, f, n) for n, f in zip(native, foreign))
    )
    local_x0, local_x1, local_y0, local_y1 = planes(
        *(jnp.where(near, n, f) for n, f in zip(native, foreign))
    )

    def params(mebibytes):
        return pltpu.CompilerParams(vmem_limit_bytes=mebibytes * 2**20)

    def columns_of(array):
        return pl.BlockSpec((array.shape[0], tile), lambda j: (0, j))

    def whole(*shape):
        return pl.BlockSpec(
            shape, lambda j: (0,) * len(shape), pipeline_mode=pl.Buffered(1)
        )

    grid = (columns // tile,)
    sums = jax.ShapeDtypeStruct((rows, columns), jnp.float32)
    tile_spec = columns_of(sums)
    slots = whole(8, half, WIDTH)
    so_far = pl.pallas_call(
        local_kernel,
        grid=grid,
        out_shape=sums,
        in_specs=[slots] * 2 + [columns_of(local), tile_spec],
        out_specs=tile_spec,
        compiler_params=params(22),
        cost_estimate=matmul_cost(rows, 8 * WIDTH, columns, rows * columns * 4),
        name="local",
    )(local_x0, local_y0, local, result_in)

    rest = 2 * (depth - first)
    so_far, left_over = pl.pallas_call(
        remote_kernel,
        grid=grid,
        out_shape=(sums, jax.ShapeDtypeStruct((rows, rest), jnp.bfloat16)),
        in_specs=[ANY] * 4 + [columns_of(same0), columns_of(relayed0), tile_spec],
        out_specs=(tile_spec, pl.BlockSpec((rows, rest), lambda j: (0, 0))),
        scratch_shapes=[
            pltpu.VMEM((rows, 2 * depth), jnp.bfloat16),
            pltpu.SemaphoreType.DMA((32,)),
        ],
        compiler_params=params(22),
        cost_estimate=matmul_cost(rows, 2 * first, columns, rows * columns * 8),
        input_output_aliases={6: 0},
        name="remote",
    )(remote_x0, remote_x1, remote_y0, remote_y1, same0, relayed0, so_far)

    corrected, power = pl.pallas_call(
        final_kernel,
        grid=grid,
        out_shape=(sums, jax.ShapeDtypeStruct((rows // 128, 128), jnp.float32)),
        in_specs=[slots] * 2
        + [columns_of(local), whole(rows, rest), columns_of(same1), columns_of(relayed1)]
        + [tile_spec],
        out_specs=(tile_spec, pl.BlockSpec((rows // 128, 128), lambda j: (0, 0))),
        scratch_shapes=[pltpu.VMEM((rows, 128), jnp.float32)],
        compiler_params=params(22),
        cost_estimate=matmul_cost(rows, 8 * WIDTH + rest, columns, rows * columns * 12),
        input_output_aliases={6: 0},
        name="final",
    )(local_x1, local_y1, local, left_over, same1, relayed1, so_far)

    line = lax.axis_size(("hi", "y", "x"))
    copies = jnp.broadcast_to(power, (line, *power.shape))
    powers = lax.all_to_all(copies, ("hi", "y", "x"), split_axis=0, concat_axis=0, tiled=True)

    scale_spec = pl.BlockSpec((rows, tile), lambda j: (0, j))
    return pl.pallas_call(
        functools.partial(scale_kernel, columns * line),
        grid=(columns // tile,),
        out_shape=jax.ShapeDtypeStruct((rows, columns), jnp.float32),
        in_specs=[pl.BlockSpec(powers.shape, lambda j: (0, 0, 0)), scale_spec],
        out_specs=scale_spec,
        scratch_shapes=[pltpu.VMEM((128, 128), jnp.float32)],
        compiler_params=params(22),
        name="scale",
    )(powers, corrected)


def solution(mesh):
    parts = Mesh(mesh.devices.reshape(2, 2, 2, 4, 4), ("lo", "c", "hi", "y", "x"))
    spec = P(("lo", "c"), ("hi", "y", "x"))

    return jax.shard_map(
        shards, mesh=parts, in_specs=(spec, spec, spec, P()), out_specs=spec, check_vma=False
    )
```
